8 devices in a mesh: dp: 1 (over z), sp: 2 (over y), cp: 4 (over x, core).
Axes of the slice: x: 2, y: 2, z: 1, core: 2. Of those that a mesh axis runs over, the one named last changes fastest.
Arguments:
- x_chunk: bfloat16 [512, 16384], P(('dp', 'sp', 'cp'))
- k_cache: bfloat16 [32768, 8, 128], P(('dp', 'sp', 'cp'))
- v_cache: bfloat16 [32768, 8, 128], P(('dp', 'sp', 'cp'))
- w_q: bfloat16 [16384, 16384], replicated
- w_k: bfloat16 [16384, 1024], replicated
- w_v: bfloat16 [16384, 1024], replicated
- w_o: bfloat16 [16384, 16384], replicated
Outputs:
- output 1: bfloat16 [512, 16384], P(('dp', 'sp', 'cp'))
- output 2: bfloat16 [512, 8, 128], P(('dp', 'sp', 'cp'))
- output 3: bfloat16 [512, 8, 128], P(('dp', 'sp', 'cp'))
All inputs are finite; a program needn't handle non-finite values.
Results may differ from the reference program's by a relative error of at most 0.00585936.
Values are sent between devices in bfloat16 or wider.
A program may use at most 4.5 GiB of HBM per device.

```python
import math
import jax
import jax.numpy as jnp
from jax import lax

D_MODEL = 16384
HEADS = 128
KV_HEADS = 8
HEAD = 128
TOK = 512
CACHE = 32768
SHARDS = 8
QBLOCK = 16
ROPE_BASE = 500000


def rope_tables(positions):
    inv_freq = 1.0 / (ROPE_BASE ** (jnp.arange(0, HEAD, 2, dtype=jnp.float32) / HEAD))
    angles = positions.astype(jnp.float32)[:, None] * inv_freq[None, :]
    return jnp.cos(angles), jnp.sin(angles)


def apply_rope(values, cos_t, sin_t):
    half_dim = HEAD // 2
    lo_half = values[..., :half_dim].astype(jnp.float32)
    hi_half = values[..., half_dim:].astype(jnp.float32)
    return jnp.concatenate([lo_half * cos_t - hi_half * sin_t, hi_half * cos_t + lo_half * sin_t], axis=-1).astype(jnp.bfloat16)


def setup_inputs(seed: int = 0, part: int = 0) -> dict:
    group_size = HEADS // KV_HEADS
    shard_len = CACHE // SHARDS
    score_gap = max(1.0, math.log(CACHE / TOK) + 1.0)
    shared_keys = jax.random.split(jax.random.key(seed), 7)
    part_keys = jax.random.split(jax.random.fold_in(jax.random.key(seed + 1), part), 5)
    x_mean = 0.6 * jax.random.normal(shared_keys[0], (D_MODEL,), jnp.float32)
    low_dims = (jnp.arange(HEAD) % (HEAD // 2)) >= (HEAD // 2 - 8)
    bias_dir = jax.random.normal(shared_keys[1], (KV_HEADS, HEAD), jnp.float32) * low_dims
    bias_kv = bias_dir / jnp.linalg.norm(bias_dir, axis=-1, keepdims=True) * math.sqrt(score_gap * math.sqrt(HEAD))
    bias_q = jnp.repeat(bias_kv, group_size, axis=0).reshape(HEADS * HEAD)
    mean_lift = x_mean[:, None] / jnp.sum(x_mean * x_mean)
    w_q = jax.random.normal(shared_keys[2], (D_MODEL, HEADS * HEAD), jnp.float32) * D_MODEL ** -0.5 + mean_lift * bias_q[None, :]
    w_k = jax.random.normal(shared_keys[3], (D_MODEL, KV_HEADS * HEAD), jnp.float32) * D_MODEL ** -0.5 + mean_lift * bias_kv.reshape(KV_HEADS * HEAD)[None, :]
    w_v = jax.random.normal(shared_keys[4], (D_MODEL, KV_HEADS * HEAD), jnp.float32) * D_MODEL ** -0.5
    w_o = jax.random.normal(shared_keys[5], (HEADS * HEAD, D_MODEL), jnp.float32) * (HEADS * HEAD) ** -0.5
    x_chunk = 0.8 * jax.random.normal(part_keys[0], (TOK, D_MODEL), jnp.float32) + x_mean[None, :]
    key_scale = jnp.exp(jax.random.uniform(part_keys[1], (SHARDS, 1, 1, 1), jnp.float32, -0.7, 0.7)) / math.sqrt(1.0 + score_gap / math.sqrt(HEAD))
    k_cache = (jax.random.normal(part_keys[2], (SHARDS, shard_len, KV_HEADS, HEAD), jnp.float32) * key_scale).reshape(CACHE, KV_HEADS, HEAD)
    val_mean = jax.random.normal(part_keys[3], (SHARDS, 1, KV_HEADS, HEAD), jnp.float32)
    v_cache = (0.5 * jax.random.normal(part_keys[4], (SHARDS, shard_len, KV_HEADS, HEAD), jnp.float32) + val_mean).reshape(CACHE, KV_HEADS, HEAD)
    return {'x_chunk': x_chunk.astype(jnp.bfloat16), 'k_cache': k_cache.astype(jnp.bfloat16), 'v_cache': v_cache.astype(jnp.bfloat16), 'w_q': w_q.astype(jnp.bfloat16), 'w_k': w_k.astype(jnp.bfloat16), 'w_v': w_v.astype(jnp.bfloat16), 'w_o': w_o.astype(jnp.bfloat16)}


def reference(x_chunk, k_cache, v_cache, w_q, w_k, w_v, w_o):
    group_size = HEADS // KV_HEADS
    attn_scale = HEAD ** -0.5
    cos_t, sin_t = rope_tables(CACHE + jnp.arange(TOK))
    q_rows = jnp.dot(x_chunk, w_q, preferred_element_type=jnp.float32).astype(jnp.bfloat16)
    q_heads = apply_rope(q_rows.reshape(TOK, KV_HEADS, group_size, HEAD), cos_t[:, None, None, :], sin_t[:, None, None, :])
    k_rows = jnp.dot(x_chunk, w_k, preferred_element_type=jnp.float32).astype(jnp.bfloat16)
    k_new = apply_rope(k_rows.reshape(TOK, KV_HEADS, HEAD), cos_t[:, None, :], sin_t[:, None, :])
    v_new = jnp.dot(x_chunk, w_v, preferred_element_type=jnp.float32).astype(jnp.bfloat16).reshape(TOK, KV_HEADS, HEAD)
    keys_all = jnp.concatenate([k_cache, k_new], axis=0)
    vals_all = jnp.concatenate([v_cache, v_new], axis=0)
    key_pos = jnp.arange(CACHE + TOK)
    block_starts = jnp.arange(TOK // QBLOCK) * QBLOCK

    def per_head(head_args):
        q_head, k_head, v_head = head_args
        k_trans = k_head.T

        def per_block(block_args):
            q_block, row_start = block_args
            scores = jnp.dot(q_block.reshape(QBLOCK * group_size, HEAD), k_trans, preferred_element_type=jnp.float32)
            scores = scores.reshape(QBLOCK, group_size, CACHE + TOK) * attn_scale
            allowed = key_pos[None, None, :] <= (CACHE + row_start + jnp.arange(QBLOCK))[:, None, None]
            scores = jnp.where(allowed, scores, -jnp.inf)
            row_max = jnp.max(scores, axis=-1, keepdims=True)
            exp_scores = jnp.exp(scores - row_max)
            row_sum = jnp.sum(exp_scores, axis=-1, keepdims=True)
            out_block = jnp.dot(exp_scores.astype(jnp.bfloat16).reshape(QBLOCK * group_size, CACHE + TOK), v_head, preferred_element_type=jnp.float32)
            return out_block.reshape(QBLOCK, group_size, HEAD) / row_sum

        blocks = lax.map(per_block, (q_head.reshape(TOK // QBLOCK, QBLOCK, group_size, HEAD), block_starts))
        return blocks.reshape(TOK, group_size, HEAD)

    attn_out = lax.map(per_head, (jnp.transpose(q_heads, (1, 0, 2, 3)), jnp.transpose(keys_all, (1, 0, 2)), jnp.transpose(vals_all, (1, 0, 2))))
    attn_rows = jnp.transpose(attn_out, (1, 0, 2, 3)).reshape(TOK, HEADS * HEAD).astype(jnp.bfloat16)
    y_out = jnp.dot(attn_rows, w_o, preferred_element_type=jnp.float32).astype(jnp.bfloat16)
    return (y_out, k_new, v_new)
```

```python
import functools
import jax
import jax.numpy as jnp
from jax import lax
from jax.experimental import pallas as pl
from jax.experimental.pallas import tpu as pltpu
from jax.sharding import PartitionSpec as P

ROPE_BASE = 500000
HD = 128
LOG2E = 1.4426950408889634
FLIPS = ((0, 0, 0), (0, 0, 1), (0, 1, 0), (1, 0, 0), (0, 1, 1), (1, 0, 1), (1, 1, 0), (1, 1, 1))


def rope_tables(positions):
    inv_freq = 1.0 / (ROPE_BASE ** (jnp.arange(0, HD, 2, dtype=jnp.float32) / HD))
    angles = positions.astype(jnp.float32)[:, None] * inv_freq[None, :]
    cos_t, sin_t = jnp.cos(angles), jnp.sin(angles)
    return jnp.concatenate([cos_t, cos_t], 1), jnp.concatenate([-sin_t, sin_t], 1)


def mm_kernel(off_ref, x_ref, w_ref, cos_ref, sin_ref, o_ref, *, rope, trans):
    acc = jnp.dot(x_ref[...], w_ref[...], preferred_element_type=jnp.float32).astype(jnp.bfloat16)
    if not rope:
        o_ref[...] = acc
        return
    for h in range(acc.shape[1] // HD):
        part = acc[:, h * HD:(h + 1) * HD].astype(jnp.float32)
        part = part * cos_ref[...] + pltpu.roll(part, HD // 2, 1) * sin_ref[...]
        if trans:
            o_ref[h * HD:(h + 1) * HD, :] = part.T.astype(jnp.bfloat16)
        else:
            o_ref[:, h * HD:(h + 1) * HD] = part.astype(jnp.bfloat16)


def matmul(x, w, cos_t, sin_t, off, n_cols, *, rope, trans=False, bn=256):
    rows, depth = x.shape
    out = (n_cols, rows) if trans else (rows, n_cols)
    ospec = pl.BlockSpec((bn, rows), lambda n, o: (n, 0)) if trans else pl.BlockSpec((rows, bn), lambda n, o: (0, n))
    return pl.pallas_call(
        functools.partial(mm_kernel, rope=rope, trans=trans),
        grid_spec=pltpu.PrefetchScalarGridSpec(
            num_scalar_prefetch=1,
            grid=(n_cols // bn,),
            in_specs=[
                pl.BlockSpec((rows, depth), lambda n, o: (0, 0), pipeline_mode=pl.Buffered(1)),
                pl.BlockSpec((depth, bn), lambda n, o: (0, o[0] + n)),
                pl.BlockSpec((rows, HD), lambda n, o: (0, 0)),
                pl.BlockSpec((rows, HD), lambda n, o: (0, 0)),
            ],
            out_specs=ospec,
        ),
        out_shape=jax.ShapeDtypeStruct(out, jnp.bfloat16),
        compiler_params=pltpu.CompilerParams(vmem_limit_bytes=48 << 20),
        cost_estimate=pl.CostEstimate(flops=2 * rows * depth * n_cols, bytes_accessed=2 * depth * n_cols, transcendentals=0),
    )(off, x, w, cos_t, sin_t)


def attn_kernel(kh_ref, vh_ref, qt_ref, kn_ref, vn_ref, o_ref,
                kb, vb, sbuf, acc, mst, lst, ksend, krecv, vsend, vrecv, *, tok, group, kblk, scale):
    cache = kb.shape[1]
    nsub = cache // kblk
    sp, cp = lax.axis_index('sp'), lax.axis_index('cp')
    chip, core = cp // 2, cp % 2
    cexp = scale * LOG2E

    def flip(v, f):
        return 1 - v if f else v

    def partner(p):
        fs, fx, fc = FLIPS[p]
        return flip(sp, fs), flip(chip, fx) * 2 + flip(core, fc)

    def dev(p):
        s, c = partner(p)
        return {'sp': s, 'cp': c}

    barrier = pltpu.get_barrier_semaphore()
    for p in range(1, 8):
        pl.semaphore_signal(barrier, inc=1, device_id=dev(p), device_id_type=pl.DeviceIdType.MESH)
    own = 2 * cp + sp
    k0 = pltpu.make_async_copy(kh_ref.at[own], kb.at[0], krecv.at[0])
    v0 = pltpu.make_async_copy(vh_ref.at[own], vb.at[0], vrecv.at[0])
    k0.start()
    v0.start()
    pl.semaphore_wait(barrier, 7)

    def remote(p):
        s, c = partner(p)
        head = 2 * c + s
        ck = pltpu.make_async_remote_copy(kh_ref.at[head], kb.at[p], ksend.at[p], krecv.at[p],
                                          device_id=dev(p), device_id_type=pl.DeviceIdType.MESH)
        cv = pltpu.make_async_remote_copy(vh_ref.at[head], vb.at[p], vsend.at[p], vrecv.at[p],
                                          device_id=dev(p), device_id_type=pl.DeviceIdType.MESH)
        return ck, cv

    for p in range(1, 8):
        ck, cv = remote(p)
        ck.start()
        cv.start()

    def q_of(h):
        return qt_ref[pl.ds(pl.multiple_of(h * HD, HD), HD), :]

    kpos = lax.broadcasted_iota(jnp.int32, (tok, tok), 0)
    qpos = lax.broadcasted_iota(jnp.int32, (tok, tok), 1)

    def first(h, carry):
        s = jnp.dot(kn_ref[...], q_of(h), preferred_element_type=jnp.float32)
        s = jnp.where(kpos <= qpos, s, -jnp.inf)
        m = jnp.max(s, axis=0, keepdims=True)
        p = jnp.exp2((s - m) * cexp)
        lst[h] = jnp.sum(p.reshape(tok // 8, 8, tok), axis=0)
        mst[h] = jnp.broadcast_to(m, (8, tok))
        acc[h] = jnp.dot(vn_ref[...], p.astype(jnp.bfloat16), preferred_element_type=jnp.float32)
        return carry

    lax.fori_loop(0, group, first, 0)

    def scores(slot, j, h, dst):
        keys = kb[slot, pl.ds(j * kblk, kblk), :]
        sbuf[dst] = jnp.dot(keys, q_of(h), preferred_element_type=jnp.float32)

    k0.wait()
    v0.wait()
    scores(0, 0, 0, 0)

    def step(i, carry):
        slot, h = i // group, i % group
        nxt = jnp.minimum(i + 1, 8 * group - 1)
        nslot, nh = nxt // group, nxt % group

        @pl.when((h == group - 1) & (slot < 7))
        def _():
            pltpu.make_async_copy(kb.at[nslot], kb.at[nslot], krecv.at[nslot]).wait()
            pltpu.make_async_copy(vb.at[nslot], vb.at[nslot], vrecv.at[nslot]).wait()

        m_run = mst[h, 0:1, :]
        l_run = lst[h]
        o_run = acc[h]
        for j in range(nsub):
            if j + 1 < nsub:
                scores(slot, j + 1, h, (j + 1) % 2)
            else:
                scores(nslot, 0, nh, (j + 1) % 2)
            s = sbuf[j % 2]
            m_new = jnp.maximum(m_run, jnp.max(s, axis=0, keepdims=True))
            alpha = jnp.exp2((m_run - m_new) * cexp)
            p = jnp.exp2((s - m_new) * cexp)
            l_run = l_run * alpha + jnp.sum(p.reshape(kblk // 8, 8, tok), axis=0)
            o_run = o_run * alpha + jnp.dot(vb[slot, :, pl.ds(j * kblk, kblk)], p.astype(jnp.bfloat16),
                                            preferred_element_type=jnp.float32)
            m_run = m_new
        mst[h] = jnp.broadcast_to(m_run, (8, tok))
        lst[h] = l_run
        acc[h] = o_run
        return carry

    lax.fori_loop(0, 8 * group, step, 0)

    def last(h, carry):
        total = jnp.sum(lst[h], axis=0, keepdims=True)
        o = acc[h] / total
        o_ref[:, pl.ds(pl.multiple_of(h * HD, HD), HD)] = o.T.astype(jnp.bfloat16)
        return carry

    lax.fori_loop(0, group, last, 0)
    for p in range(1, 8):
        ck, cv = remote(p)
        ck.wait_send()
        cv.wait_send()


def attention(kh, vh, qt, kn, vnt, kblk=512):
    n_kv, cache, _ = kh.shape
    group, tok = qt.shape[0] // HD, qt.shape[1]
    return pl.pallas_call(
        functools.partial(attn_kernel, tok=tok, group=group, kblk=kblk, scale=HD ** -0.5),
        in_specs=[pl.BlockSpec(memory_space=pl.ANY), pl.BlockSpec(memory_space=pl.ANY)] + [pl.BlockSpec(memory_space=pltpu.VMEM)] * 3,
        out_specs=pl.BlockSpec(memory_space=pltpu.VMEM),
        out_shape=jax.ShapeDtypeStruct((tok, group * HD), jnp.bfloat16),
        scratch_shapes=[
            pltpu.VMEM((8, cache, HD), jnp.bfloat16),
            pltpu.VMEM((8, HD, cache), jnp.bfloat16),
            pltpu.VMEM((2, kblk, tok), jnp.float32),
            pltpu.VMEM((group, HD, tok), jnp.float32),
            pltpu.VMEM((group, 8, tok), jnp.float32),
            pltpu.VMEM((group, 8, tok), jnp.float32),
            pltpu.SemaphoreType.DMA((8,)),
            pltpu.SemaphoreType.DMA((8,)),
            pltpu.SemaphoreType.DMA((8,)),
            pltpu.SemaphoreType.DMA((8,)),
        ],
        compiler_params=pltpu.CompilerParams(collective_id=0, has_side_effects=True, vmem_limit_bytes=60 << 20),
    )(kh, vh, qt, kn, vnt)


def solution(mesh):
    cp_size = mesh.shape['cp']
    row_spec = P(('dp', 'sp', 'cp'))

    def local_fn(x_loc, kc_loc, vc_loc, w_q, w_k, w_v, w_o):
        cache_loc, n_kv, _ = kc_loc.shape
        seq_size = mesh.shape['sp'] * cp_size
        sp, cp = lax.axis_index('sp'), lax.axis_index('cp')
        rows = x_loc.shape[0] * cp_size
        x_g = lax.all_gather(x_loc, 'cp', axis=0, tiled=True)
        cos_t, sin_t = rope_tables(cache_loc * seq_size + sp * rows + jnp.arange(rows))
        kh = jnp.transpose(kc_loc, (1, 0, 2))
        vh = jnp.transpose(vc_loc, (1, 2, 0))
        q_cols = w_q.shape[1] // cp_size
        k_cols = w_k.shape[1] // cp_size
        qoff = jnp.reshape(cp * (q_cols // 256), (1,)).astype(jnp.int32)
        koff = jnp.reshape(cp * (k_cols // 256), (1,)).astype(jnp.int32)
        k_part = matmul(x_g, w_k, cos_t, sin_t, koff, k_cols, rope=True)
        v_part = matmul(x_g, w_v, cos_t, sin_t, koff, k_cols, rope=False)
        qt = matmul(x_g, w_q, cos_t, sin_t, qoff, q_cols, rope=True, trans=True)
        kv = jnp.stack([k_part, v_part], 0)
        kv_rows = lax.all_to_all(kv, 'cp', split_axis=1, concat_axis=2, tiled=True)
        k_new = kv_rows[0].reshape(x_loc.shape[0], n_kv, HD)
        v_new = kv_rows[1].reshape(x_loc.shape[0], n_kv, HD)
        kv_head = lax.all_to_all(kv, 'sp', split_axis=2, concat_axis=1, tiled=True)
        qt = lax.all_to_all(qt, 'sp', split_axis=0, concat_axis=1, tiled=True)
        o = attention(kh, vh, qt, kv_head[0], kv_head[1].T)
        o = lax.all_to_all(o, 'sp', split_axis=0, concat_axis=1, tiled=True)
        o_g = lax.all_gather(o, 'cp', axis=1, tiled=True)
        y = matmul(o_g, w_o, cos_t, sin_t, qoff, q_cols, rope=False)
        y_loc = lax.all_to_all(y, 'cp', split_axis=0, concat_axis=1, tiled=True)
        return y_loc, k_new, v_new

    return jax.shard_map(local_fn, mesh=mesh, in_specs=(row_spec, row_spec, row_spec, P(), P(), P(), P()), out_specs=(row_spec, row_spec, row_spec), check_vma=False)
```

```python
import functools
import jax
import jax.numpy as jnp
from jax import lax
from jax.experimental import pallas as pl
from jax.experimental.pallas import tpu as pltpu
from jax.sharding import PartitionSpec as P

ROPE_BASE = 500000
HD = 128
BN_Q = 256
BN_O = 256
LOG2E = 1.4426950408889634
FLIPS = ((0, 0, 0), (0, 0, 1), (0, 1, 0), (1, 0, 0), (0, 1, 1), (1, 0, 1), (1, 1, 0), (1, 1, 1))


def rope_tables(positions):
    inv_freq = 1.0 / (ROPE_BASE ** (jnp.arange(0, HD, 2, dtype=jnp.float32) / HD))
    angles = positions.astype(jnp.float32)[:, None] * inv_freq[None, :]
    cos_t, sin_t = jnp.cos(angles), jnp.sin(angles)
    return jnp.concatenate([cos_t, cos_t], 1), jnp.concatenate([-sin_t, sin_t], 1)


def mm_kernel(off_ref, x_ref, w_ref, cos_ref, sin_ref, o_ref, *, rope, trans):
    acc = jnp.dot(x_ref[...], w_ref[...], preferred_element_type=jnp.float32).astype(jnp.bfloat16)
    if not rope:
        o_ref[...] = acc
        return
    for h in range(acc.shape[1] // HD):
        part = acc[:, h * HD:(h + 1) * HD].astype(jnp.float32)
        part = part * cos_ref[...] + pltpu.roll(part, HD // 2, 1) * sin_ref[...]
        if trans:
            o_ref[h * HD:(h + 1) * HD, :] = part.T.astype(jnp.bfloat16)
        else:
            o_ref[:, h * HD:(h + 1) * HD] = part.astype(jnp.bfloat16)


def matmul(x, w, cos_t, sin_t, off, n_cols, *, rope, trans=False, bn=256):
    rows, depth = x.shape
    out = (n_cols, rows) if trans else (rows, n_cols)
    ospec = pl.BlockSpec((bn, rows), lambda n, o: (n, 0)) if trans else pl.BlockSpec((rows, bn), lambda n, o: (0, n))
    return pl.pallas_call(
        functools.partial(mm_kernel, rope=rope, trans=trans),
        grid_spec=pltpu.PrefetchScalarGridSpec(
            num_scalar_prefetch=1,
            grid=(n_cols // bn,),
            in_specs=[
                pl.BlockSpec((rows, depth), lambda n, o: (0, 0), pipeline_mode=pl.Buffered(1)),
                pl.BlockSpec((depth, bn), lambda n, o: (0, o[0] + n)),
                pl.BlockSpec((rows, HD), lambda n, o: (0, 0)),
                pl.BlockSpec((rows, HD), lambda n, o: (0, 0)),
            ],
            out_specs=ospec,
        ),
        out_shape=jax.ShapeDtypeStruct(out, jnp.bfloat16),
        compiler_params=pltpu.CompilerParams(vmem_limit_bytes=48 << 20),
        cost_estimate=pl.CostEstimate(flops=2 * rows * depth * n_cols, bytes_accessed=2 * depth * n_cols, transcendentals=0),
    )(off, x, w, cos_t, sin_t)


def attn_kernel(kh_ref, vh_ref, qt_ref, kn_ref, vn_ref, og_ref,
                kb, vb, sbuf, acc, mst, lst, ost, ksend, krecv, vsend, vrecv,
                osend, orecv, fsend, frecv, *, tok, group, kblk, scale):
    cache = kb.shape[1]
    nsub = cache // kblk
    half = tok // 2
    width = group * HD
    sp, cp = lax.axis_index('sp'), lax.axis_index('cp')
    chip, core = cp // 2, cp % 2
    cexp = scale * LOG2E
    own = 2 * cp + sp

    def flip(v, f):
        return 1 - v if f else v

    def partner(p):
        fs, fx, fc = FLIPS[p]
        return flip(sp, fs), flip(chip, fx) * 2 + flip(core, fc)

    def dev(p):
        s, c = partner(p)
        return {'sp': s, 'cp': c}

    def head_of(p):
        s, c = partner(p)
        return 2 * c + s

    barrier = pltpu.get_barrier_semaphore()
    for p in range(1, 8):
        pl.semaphore_signal(barrier, inc=1, device_id=dev(p), device_id_type=pl.DeviceIdType.MESH)
    k0 = pltpu.make_async_copy(kh_ref.at[own], kb.at[0], krecv.at[0])
    v0 = pltpu.make_async_copy(vh_ref.at[own], vb.at[0], vrecv.at[0])
    k0.start()
    v0.start()
    pl.semaphore_wait(barrier, 7)

    def remote(p):
        ck = pltpu.make_async_remote_copy(kh_ref.at[head_of(p)], kb.at[p], ksend.at[p], krecv.at[p],
                                          device_id=dev(p), device_id_type=pl.DeviceIdType.MESH)
        cv = pltpu.make_async_remote_copy(vh_ref.at[head_of(p)], vb.at[p], vsend.at[p], vrecv.at[p],
                                          device_id=dev(p), device_id_type=pl.DeviceIdType.MESH)
        return ck, cv

    for p in range(1, 8):
        ck, cv = remote(p)
        ck.start()
        cv.start()

    def q_of(h):
        return qt_ref[pl.ds(pl.multiple_of(h * HD, HD), HD), :]

    kpos = lax.broadcasted_iota(jnp.int32, (tok, tok), 0)
    qpos = lax.broadcasted_iota(jnp.int32, (tok, tok), 1)

    def first(h, carry):
        s = jnp.dot(kn_ref[...], q_of(h), preferred_element_type=jnp.float32)
        s = jnp.where(kpos <= qpos, s, -jnp.inf)
        m = jnp.max(s, axis=0, keepdims=True)
        p = jnp.exp2((s - m) * cexp)
        lst[h] = jnp.sum(p.reshape(tok // 8, 8, tok), axis=0)
        mst[h] = jnp.broadcast_to(m, (8, tok))
        acc[h] = jnp.dot(vn_ref[...], p.astype(jnp.bfloat16), preferred_element_type=jnp.float32)
        return carry

    lax.fori_loop(0, group, first, 0)

    def scores(slot, j, h, dst):
        s = jnp.dot(kb[slot, pl.ds(j * kblk, kblk), :], q_of(h), preferred_element_type=jnp.float32)
        sbuf[dst] = s
        return jnp.max(s.reshape(kblk // 8, 8, tok), axis=0)

    def out_copies(h):
        cols = pl.ds(pl.multiple_of(h * HD, HD), HD)
        dcols = pl.ds(pl.multiple_of(own * width + h * HD, HD), HD)
        res = [pltpu.make_async_copy(ost.at[pl.ds(sp * half, half), cols], og_ref.at[:, dcols], osend.at[0])]
        for p in (1, 2, 3, 6):
            g = flip(sp, FLIPS[p][0])
            res.append(pltpu.make_async_remote_copy(
                ost.at[pl.ds(g * half, half), cols], og_ref.at[:, dcols], osend.at[p], orecv.at[p],
                device_id=dev(p), device_id_type=pl.DeviceIdType.MESH))
        return res

    def send_out(h):
        for c in out_copies(h):
            c.start()

    k0.wait()
    v0.wait()
    m_first = scores(0, 0, 0, 0)

    def step(i, m_ahead):
        slot, h = i // group, i % group
        nxt = jnp.minimum(i + 1, 8 * group - 1)
        nslot, nh = nxt // group, nxt % group

        @pl.when((h == group - 1) & (slot < 7))
        def _():
            pltpu.make_async_copy(kb.at[nslot], kb.at[nslot], krecv.at[nslot]).wait()
            pltpu.make_async_copy(vb.at[nslot], vb.at[nslot], vrecv.at[nslot]).wait()

        @pl.when((slot == 7) & (h > 0))
        def _():
            send_out(h - 1)

        m_run = mst[h, 0:1, :]
        l_run = lst[h]
        o_run = acc[h]
        for j in range(nsub):
            m_blk = m_ahead
            if j + 1 < nsub:
                m_ahead = scores(slot, j + 1, h, (j + 1) % 2)
            else:
                m_ahead = scores(nslot, 0, nh, (j + 1) % 2)
            m_new = jnp.maximum(m_run, jnp.max(m_blk, axis=0, keepdims=True))
            alpha = jnp.exp2((m_run - m_new) * cexp)
            p = jnp.exp2((sbuf[j % 2] - m_new) * cexp)
            l_run = l_run * alpha + jnp.sum(p.reshape(kblk // 8, 8, tok), axis=0)
            o_run = o_run * alpha + jnp.dot(vb[slot, :, pl.ds(j * kblk, kblk)], p.astype(jnp.bfloat16),
                                            preferred_element_type=jnp.float32)
            m_run = m_new
        mst[h] = jnp.broadcast_to(m_run, (8, tok))
        lst[h] = l_run
        acc[h] = o_run

        @pl.when(slot == 7)
        def _():
            o = acc[h] / jnp.sum(lst[h], axis=0, keepdims=True)
            ost[:, pl.ds(pl.multiple_of(h * HD, HD), HD)] = o.T.astype(jnp.bfloat16)

        return m_ahead

    lax.fori_loop(0, 8 * group, step, m_first)
    for p in range(1, 8):
        ck, cv = remote(p)
        ck.wait_send()
        cv.wait_send()
    send_out(group - 1)

    def cols_of(p):
        return og_ref.at[:, pl.ds(pl.multiple_of(head_of(p) * width, width), width)]

    def forward(n, p):
        return pltpu.make_async_remote_copy(cols_of(p), cols_of(p), fsend.at[n], frecv.at[n],
                                            device_id=dev(1), device_id_type=pl.DeviceIdType.MESH)

    for n, p in enumerate((3, 2, 6)):
        pltpu.make_async_copy(cols_of(p), cols_of(p), orecv.at[p]).wait()
        forward(n, p).start()
    pltpu.make_async_copy(cols_of(1), cols_of(1), orecv.at[1]).wait()
    for p in (0, 1, 2, 3, 6):
        pltpu.make_async_copy(ost.at[pl.ds(0, half), :], ost.at[pl.ds(0, half), :], osend.at[p]).wait()
    for n, p in enumerate((3, 2, 6)):
        forward(n, p).wait()


def attention(kh, vh, qt, kn, vnt, kblk=2048):
    n_kv, cache, _ = kh.shape
    group, tok = qt.shape[0] // HD, qt.shape[1]
    return pl.pallas_call(
        functools.partial(attn_kernel, tok=tok, group=group, kblk=kblk, scale=HD ** -0.5),
        in_specs=[pl.BlockSpec(memory_space=pl.ANY), pl.BlockSpec(memory_space=pl.ANY)] + [pl.BlockSpec(memory_space=pltpu.VMEM)] * 3,
        out_specs=pl.BlockSpec(memory_space=pl.ANY),
        out_shape=jax.ShapeDtypeStruct((tok // 2, n_kv * group * HD), jnp.bfloat16),
        scratch_shapes=[
            pltpu.VMEM((8, cache, HD), jnp.bfloat16),
            pltpu.VMEM((8, HD, cache), jnp.bfloat16),
            pltpu.VMEM((2, kblk, tok), jnp.float32),
            pltpu.VMEM((group, HD, tok), jnp.float32),
            pltpu.VMEM((group, 8, tok), jnp.float32),
            pltpu.VMEM((group, 8, tok), jnp.float32),
            pltpu.VMEM((tok, group * HD), jnp.bfloat16),
        ] + [pltpu.SemaphoreType.DMA((8,))] * 6 + [pltpu.SemaphoreType.DMA((3,))] * 2,
        compiler_params=pltpu.CompilerParams(collective_id=0, has_side_effects=True, vmem_limit_bytes=62 << 20),
    )(kh, vh, qt, kn, vnt)


def oproj_kernel(x_hbm, w_hbm, y_hbm, x_ref, wbuf, yst, xsem, wsem, ysend, yrecv, *, bn, rows):
    sp, cp = lax.axis_index('sp'), lax.axis_index('cp')
    chip, core = cp // 2, cp % 2
    steps = yst.shape[0]
    base = cp * (steps * bn)

    def dev(f):
        c = (1 - chip if f // 2 else chip) * 2 + (1 - core if f % 2 else core)
        return c, {'sp': sp, 'cp': c}

    barrier = pltpu.get_barrier_semaphore()
    for f in range(1, 4):
        pl.semaphore_signal(barrier, inc=1, device_id=dev(f)[1], device_id_type=pl.DeviceIdType.MESH)

    def wcopy(n, slot):
        cols = pl.ds(pl.multiple_of(base + n * bn, bn), bn)
        return pltpu.make_async_copy(w_hbm.at[:, cols], wbuf.at[slot], wsem.at[slot])

    xc = pltpu.make_async_copy(x_hbm, x_ref, xsem)
    xc.start()
    wcopy(0, 0).start()
    wcopy(1, 1).start()
    pl.semaphore_wait(barrier, 3)
    xc.wait()

    def y_copies(n):
        cols = pl.ds(pl.multiple_of(base + n * bn, bn), bn)
        res = [pltpu.make_async_copy(yst.at[n, pl.ds(cp * rows, rows), :], y_hbm.at[:, cols], ysend.at[0])]
        for f in range(1, 4):
            c, d = dev(f)
            res.append(pltpu.make_async_remote_copy(yst.at[n, pl.ds(c * rows, rows), :], y_hbm.at[:, cols], ysend.at[f], yrecv.at[f],
                                                    device_id=d, device_id_type=pl.DeviceIdType.MESH))
        return res

    def send(n):
        for c in y_copies(n):
            c.start()

    def step(n, carry):
        slot = n % 2
        wcopy(n, slot).wait()
        yst[n] = jnp.dot(x_ref[...], wbuf[slot], preferred_element_type=jnp.float32).astype(jnp.bfloat16)

        @pl.when(n + 2 < steps)
        def _():
            wcopy(n + 2, slot).start()

        @pl.when(n > 0)
        def _():
            send(n - 1)

        return carry

    lax.fori_loop(0, steps, step, 0)
    send(steps - 1)
    width = steps * bn
    for f in range(4):
        c, _ = dev(f)
        mine = y_hbm.at[:, pl.ds(pl.multiple_of(c * width, width), width)]
        pltpu.make_async_copy(mine, mine, ysend.at[f]).wait()
        if f:
            pltpu.make_async_copy(mine, mine, yrecv.at[f]).wait()


def out_project(o_g, w_o, cp_size, bn=256):
    rows, depth = o_g.shape
    n_cols = w_o.shape[1]
    steps = n_cols // cp_size // bn
    return pl.pallas_call(
        functools.partial(oproj_kernel, bn=bn, rows=rows // cp_size),
        in_specs=[pl.BlockSpec(memory_space=pl.ANY)] * 2,
        out_specs=pl.BlockSpec(memory_space=pl.ANY),
        out_shape=jax.ShapeDtypeStruct((rows // cp_size, n_cols), jnp.bfloat16),
        scratch_shapes=[
            pltpu.VMEM((rows, depth), jnp.bfloat16),
            pltpu.VMEM((2, depth, bn), jnp.bfloat16),
            pltpu.VMEM((steps, rows, bn), jnp.bfloat16),
            pltpu.SemaphoreType.DMA,
            pltpu.SemaphoreType.DMA((2,)),
            pltpu.SemaphoreType.DMA((4,)),
            pltpu.SemaphoreType.DMA((4,)),
        ],
        compiler_params=pltpu.CompilerParams(collective_id=1, has_side_effects=True, vmem_limit_bytes=60 << 20),
    )(o_g, w_o)


def solution(mesh):
    cp_size = mesh.shape['cp']
    row_spec = P(('dp', 'sp', 'cp'))

    def local_fn(x_loc, kc_loc, vc_loc, w_q, w_k, w_v, w_o):
        cache_loc, n_kv, _ = kc_loc.shape
        seq_size = mesh.shape['sp'] * cp_size
        sp, cp = lax.axis_index('sp'), lax.axis_index('cp')
        rows = x_loc.shape[0] * cp_size
        x_g = lax.all_gather(x_loc, 'cp', axis=0, tiled=True)
        cos_t, sin_t = rope_tables(cache_loc * seq_size + sp * rows + jnp.arange(rows))
        kh = jnp.transpose(kc_loc, (1, 0, 2))
        vh = jnp.transpose(vc_loc, (1, 2, 0))
        x_g, kh, vh = lax.optimization_barrier((x_g, kh, vh))
        q_cols = w_q.shape[1] // cp_size
        k_cols = w_k.shape[1] // cp_size
        qoff = jnp.reshape(cp * (q_cols // BN_Q), (1,)).astype(jnp.int32)
        koff = jnp.reshape(cp * (k_cols // 256), (1,)).astype(jnp.int32)
        k_part = matmul(x_g, w_k, cos_t, sin_t, koff, k_cols, rope=True)
        v_part = matmul(x_g, w_v, cos_t, sin_t, koff, k_cols, rope=False)
        qt = matmul(x_g, w_q, cos_t, sin_t, qoff, q_cols, rope=True, trans=True, bn=BN_Q)
        kv = jnp.stack([k_part, v_part], 0)
        kv_rows = lax.all_to_all(kv, 'cp', split_axis=1, concat_axis=2, tiled=True)
        k_new = kv_rows[0].reshape(x_loc.shape[0], n_kv, HD)
        v_new = kv_rows[1].reshape(x_loc.shape[0], n_kv, HD)
        kv_head = lax.all_to_all(kv, 'sp', split_axis=2, concat_axis=1, tiled=True)
        qt = lax.all_to_all(qt, 'sp', split_axis=0, concat_axis=1, tiled=True)
        o_g = attention(kh, vh, qt, kv_head[0], kv_head[1].T)
        y_loc = out_project(o_g, w_o, cp_size, BN_O)
        return y_loc, k_new, v_new

    return jax.shard_map(local_fn, mesh=mesh, in_specs=(row_spec, row_spec, row_spec, P(), P(), P(), P()), out_specs=(row_spec, row_spec, row_spec), check_vma=False)
```

```python
import functools
import jax
import jax.numpy as jnp
from jax import lax
from jax.experimental import pallas as pl
from jax.experimental.pallas import tpu as pltpu
from jax.sharding import PartitionSpec as P

ROPE_BASE = 500000
HD = 128
BN_O = 256
LOG2E = 1.4426950408889634
FLIPS = ((0, 0, 0), (0, 0, 1), (0, 1, 0), (1, 0, 0), (0, 1, 1), (1, 0, 1), (1, 1, 0), (1, 1, 1))


def rope_tables(positions):
    inv_freq = 1.0 / (ROPE_BASE ** (jnp.arange(0, HD, 2, dtype=jnp.float32) / HD))
    angles = positions.astype(jnp.float32)[:, None] * inv_freq[None, :]
    cos_t, sin_t = jnp.cos(angles), jnp.sin(angles)
    return jnp.concatenate([cos_t, cos_t], 1), jnp.concatenate([-sin_t, sin_t], 1)


def front_kernel(x_hbm, wq_hbm, wk_hbm, wv_hbm, cos_ref, sin_ref, qt_ref, kvr_hbm, kvh_hbm,
                 xg, wbuf, kvbuf, acc, kvacc, kvst, xsem, wsem, kvsem, xsend, xcore, xchip, fsend, frecv,
                 ssend, srecv, *, kblk, chunk):
    sp, cp = lax.axis_index('sp'), lax.axis_index('cp')
    chip, core = cp // 2, cp % 2
    rows, depth = x_hbm.shape
    n_cols = acc.shape[1]
    kv_cols = kvst.shape[2]
    steps, chunks = depth // kblk, depth // chunk
    per = chunk // kblk
    n_buf = wbuf.shape[0]

    def peer(f):
        return (1 - chip if f // 2 else chip) * 2 + (1 - core if f % 2 else core)

    def dev(f):
        return {'sp': sp, 'cp': peer(f)}

    other = {'sp': 1 - sp, 'cp': cp}
    barrier = pltpu.get_barrier_semaphore()
    for d in (dev(1), dev(2), dev(3), other):
        pl.semaphore_signal(barrier, inc=1, device_id=d, device_id_type=pl.DeviceIdType.MESH)

    def w_copies(k):
        slot = k % n_buf
        depth_k = pl.ds(pl.multiple_of(k * kblk, kblk), kblk)
        kv_c = pl.ds(pl.multiple_of(cp * kv_cols, kv_cols), kv_cols)
        return (pltpu.make_async_copy(wq_hbm.at[depth_k, pl.ds(pl.multiple_of(cp * n_cols, n_cols), n_cols)], wbuf.at[slot], wsem.at[slot]),
                pltpu.make_async_copy(wk_hbm.at[depth_k, kv_c], kvbuf.at[slot, 0], kvsem.at[slot, 0]),
                pltpu.make_async_copy(wv_hbm.at[depth_k, kv_c], kvbuf.at[slot, 1], kvsem.at[slot, 1]))

    def part(f, c):
        return pl.ds(pl.multiple_of(peer(f) * rows, rows), rows), pl.ds(pl.multiple_of(c * chunk, chunk), chunk)

    mine = xg.at[pl.ds(pl.multiple_of(cp * rows, rows), rows), :]
    local = pltpu.make_async_copy(x_hbm, mine, xsem)
    local.start()
    for k in range(n_buf - 1):
        for c in w_copies(k):
            c.start()
    pl.semaphore_wait(barrier, 4)

    def to_chip(c):
        return pltpu.make_async_remote_copy(x_hbm.at[:, part(0, c)[1]], xg.at[part(0, c)], xsend.at[0, c], xchip.at[c],
                                            device_id=dev(2), device_id_type=pl.DeviceIdType.MESH)

    def to_core(c):
        return pltpu.make_async_remote_copy(x_hbm.at[:, part(0, c)[1]], xg.at[part(0, c)], xsend.at[1, c], xcore.at[c],
                                            device_id=dev(1), device_id_type=pl.DeviceIdType.MESH)

    def forward(c):
        return pltpu.make_async_remote_copy(xg.at[part(2, c)], xg.at[part(2, c)], fsend.at[c], frecv.at[c],
                                            device_id=dev(1), device_id_type=pl.DeviceIdType.MESH)

    def arrived(f, c, sem):
        pltpu.make_async_copy(xg.at[part(f, c)], xg.at[part(f, c)], sem.at[c]).wait()

    for c in range(chunks):
        to_chip(c).start()
        to_core(c).start()
    acc[...] = jnp.zeros_like(acc)
    kvacc[...] = jnp.zeros_like(kvacc)
    local.wait()
    arrived(2, 0, xchip)
    forward(0).start()

    def step(k, carry):
        c = k // per

        @pl.when(k % per == 0)
        def _():
            arrived(1, c, xcore)
            arrived(3, c, frecv)

        slot = k % n_buf
        for cpy in w_copies(k):
            cpy.wait()

        @pl.when(k + n_buf - 1 < steps)
        def _():
            for cpy in w_copies(k + n_buf - 1):
                cpy.start()

        xk = xg[:, pl.ds(pl.multiple_of(k * kblk, kblk), kblk)]
        acc[...] += jnp.dot(xk, wbuf[slot], preferred_element_type=jnp.float32)
        for n in range(2):
            kvacc[n] += jnp.dot(xk, kvbuf[slot, n], preferred_element_type=jnp.float32)

        @pl.when((k % per == per // 2) & (c + 1 < chunks))
        def _():
            arrived(2, c + 1, xchip)
            forward(c + 1).start()

        return carry

    lax.fori_loop(0, steps, step, 0)

    def rope(v):
        v = v.astype(jnp.bfloat16).astype(jnp.float32)
        return v * cos_ref[...] + pltpu.roll(v, HD // 2, 1) * sin_ref[...]

    for h in range(kv_cols // HD):
        kvst[0, :, h * HD:(h + 1) * HD] = rope(kvacc[0, :, h * HD:(h + 1) * HD]).astype(jnp.bfloat16)
    kvst[1] = kvacc[1].astype(jnp.bfloat16)

    def q_head(h, carry):
        cols = pl.ds(pl.multiple_of(h * HD, HD), HD)
        qt_ref[cols, :] = rope(acc[:, cols]).T.astype(jnp.bfloat16)
        return carry

    heads = n_cols // HD
    lax.fori_loop(0, heads // 2, q_head, 0)
    all_rows = rows * 4
    dcols = pl.ds(pl.multiple_of(cp * kv_cols, kv_cols), kv_cols)
    copies = []
    for n in range(2):
        for f in range(4):
            src = kvst.at[n, pl.ds(pl.multiple_of(peer(f) * rows, rows), rows), :]
            dst = kvr_hbm.at[n, :, dcols]
            if f:
                copies.append(pltpu.make_async_remote_copy(src, dst, ssend.at[n, f], srecv.at[n, f], device_id=dev(f), device_id_type=pl.DeviceIdType.MESH))
            else:
                copies.append(pltpu.make_async_copy(src, dst, ssend.at[n, f]))
        dst = kvh_hbm.at[n, pl.ds(pl.multiple_of(sp * all_rows, all_rows), all_rows), :]
        src = kvst.at[n, :, pl.ds(pl.multiple_of(sp * HD, HD), HD)]
        copies.append(pltpu.make_async_copy(src, dst, ssend.at[n, 4]))
        src = kvst.at[n, :, pl.ds(pl.multiple_of((1 - sp) * HD, HD), HD)]
        copies.append(pltpu.make_async_remote_copy(src, dst, ssend.at[n, 5], srecv.at[n, 5], device_id=other, device_id_type=pl.DeviceIdType.MESH))
    for cpy in copies:
        cpy.start()
    lax.fori_loop(heads // 2, heads, q_head, 0)
    for c in range(chunks):
        to_chip(c).wait_send()
        to_core(c).wait_send()
        forward(c).wait_send()
    for cpy in copies:
        cpy.wait()


def front(x_loc, w_q, w_k, w_v, cos_t, sin_t, cp_size, kblk=512, chunk=2048, n_buf=4):
    rows, depth = x_loc.shape
    n_cols, kv_cols = w_q.shape[1] // cp_size, w_k.shape[1] // cp_size
    chunks = depth // chunk
    dma = pltpu.SemaphoreType.DMA
    return pl.pallas_call(
        functools.partial(front_kernel, kblk=kblk, chunk=chunk),
        in_specs=[pl.BlockSpec(memory_space=pl.ANY)] * 4 + [pl.BlockSpec(memory_space=pltpu.VMEM)] * 2,
        out_specs=[pl.BlockSpec(memory_space=pltpu.VMEM)] + [pl.BlockSpec(memory_space=pl.ANY)] * 2,
        out_shape=[
            jax.ShapeDtypeStruct((n_cols, rows * cp_size), jnp.bfloat16),
            jax.ShapeDtypeStruct((2, rows, w_k.shape[1]), jnp.bfloat16),
            jax.ShapeDtypeStruct((2, 2 * rows * cp_size, HD), jnp.bfloat16),
        ],
        scratch_shapes=[
            pltpu.VMEM((rows * cp_size, depth), jnp.bfloat16),
            pltpu.VMEM((n_buf, kblk, n_cols), jnp.bfloat16),
            pltpu.VMEM((n_buf, 2, kblk, kv_cols), jnp.bfloat16),
            pltpu.VMEM((rows * cp_size, n_cols), jnp.float32),
            pltpu.VMEM((2, rows * cp_size, kv_cols), jnp.float32),
            pltpu.VMEM((2, rows * cp_size, kv_cols), jnp.bfloat16),
            dma, dma((n_buf,)), dma((n_buf, 2)), dma((2, chunks)), dma((chunks,)), dma((chunks,)),
            dma((chunks,)), dma((chunks,)), dma((2, 6)), dma((2, 6)),
        ],
        compiler_params=pltpu.CompilerParams(collective_id=2, has_side_effects=True, vmem_limit_bytes=56 << 20),
    )(x_loc, w_q, w_k, w_v, cos_t, sin_t)


def attn_kernel(kh_ref, vh_ref, qt_ref, kn_ref, vn_ref, og_ref,
                kb, vb, sbuf, acc, mst, lst, ost, ksend, krecv, vsend, vrecv,
                osend, orecv, fsend, frecv, *, tok, group, kblk, scale):
    cache = kb.shape[1]
    nsub = cache // kblk
    half = tok // 2
    width = group * HD
    sp, cp = lax.axis_index('sp'), lax.axis_index('cp')
    chip, core = cp // 2, cp % 2
    cexp = scale * LOG2E
    own = 2 * cp + sp

    def flip(v, f):
        return 1 - v if f else v

    def partner(p):
        fs, fx, fc = FLIPS[p]
        return flip(sp, fs), flip(chip, fx) * 2 + flip(core, fc)

    def dev(p):
        s, c = partner(p)
        return {'sp': s, 'cp': c}

    def head_of(p):
        s, c = partner(p)
        return 2 * c + s

    barrier = pltpu.get_barrier_semaphore()
    for p in range(1, 8):
        pl.semaphore_signal(barrier, inc=1, device_id=dev(p), device_id_type=pl.DeviceIdType.MESH)
    k0 = pltpu.make_async_copy(kh_ref.at[own], kb.at[0], krecv.at[0])
    v0 = pltpu.make_async_copy(vh_ref.at[own], vb.at[0], vrecv.at[0])
    k0.start()
    v0.start()
    pl.semaphore_wait(barrier, 7)

    def remote(p):
        ck = pltpu.make_async_remote_copy(kh_ref.at[head_of(p)], kb.at[p], ksend.at[p], krecv.at[p],
                                          device_id=dev(p), device_id_type=pl.DeviceIdType.MESH)
        cv = pltpu.make_async_remote_copy(vh_ref.at[head_of(p)], vb.at[p], vsend.at[p], vrecv.at[p],
                                          device_id=dev(p), device_id_type=pl.DeviceIdType.MESH)
        return ck, cv

    for p in range(1, 8):
        ck, cv = remote(p)
        ck.start()
        cv.start()

    def q_of(h):
        return qt_ref[pl.ds(pl.multiple_of(h * HD, HD), HD), :]

    kpos = lax.broadcasted_iota(jnp.int32, (tok, tok), 0)
    qpos = lax.broadcasted_iota(jnp.int32, (tok, tok), 1)

    def first(h, carry):
        s = jnp.dot(kn_ref[...], q_of(h), preferred_element_type=jnp.float32)
        s = jnp.where(kpos <= qpos, s, -jnp.inf)
        m = jnp.max(s, axis=0, keepdims=True)
        p = jnp.exp2((s - m) * cexp)
        lst[h] = jnp.sum(p.reshape(tok // 8, 8, tok), axis=0)
        mst[h] = jnp.broadcast_to(m, (8, tok))
        acc[h] = jnp.dot(vn_ref[...], p.astype(jnp.bfloat16), preferred_element_type=jnp.float32)
        return carry

    lax.fori_loop(0, group, first, 0, unroll=2)

    def scores(slot, j, h, dst):
        s = jnp.dot(kb[slot, pl.ds(j * kblk, kblk), :], q_of(h), preferred_element_type=jnp.float32)
        sbuf[dst] = s
        return jnp.max(s.reshape(kblk // 8, 8, tok), axis=0)

    def out_copies(h):
        cols = pl.ds(pl.multiple_of(h * HD, HD), HD)
        dcols = pl.ds(pl.multiple_of(own * width + h * HD, HD), HD)
        res = [pltpu.make_async_copy(ost.at[pl.ds(sp * half, half), cols], og_ref.at[:, dcols], osend.at[0])]
        for p in (1, 2, 3, 6):
            g = flip(sp, FLIPS[p][0])
            res.append(pltpu.make_async_remote_copy(
                ost.at[pl.ds(g * half, half), cols], og_ref.at[:, dcols], osend.at[p], orecv.at[p],
                device_id=dev(p), device_id_type=pl.DeviceIdType.MESH))
        return res

    def send_out(h):
        for c in out_copies(h):
            c.start()

    k0.wait()
    v0.wait()
    m_first = scores(0, 0, 0, 0)

    tail = 6 * group

    def place(i):
        t = i // tail
        r = i % tail
        return (1 - t) * (i // group) + t * (6 + r % 2), (1 - t) * (i % group) + t * (r // 2)

    def step(i, m_ahead):
        slot, h = place(i)
        nslot, nh = place(jnp.minimum(i + 1, 8 * group - 1))

        @pl.when(((i % group == group - 1) & (i < tail)) | (i == tail))
        def _():
            pltpu.make_async_copy(kb.at[nslot], kb.at[nslot], krecv.at[nslot]).wait()
            pltpu.make_async_copy(vb.at[nslot], vb.at[nslot], vrecv.at[nslot]).wait()

        @pl.when((slot == 7) & (h > 0))
        def _():
            send_out(h - 1)

        m_run = mst[h, 0:1, :]
        l_run = lst[h]
        o_run = acc[h]
        for j in range(nsub):
            m_blk = m_ahead
            if j + 1 < nsub:
                m_ahead = scores(slot, j + 1, h, (j + 1) % 2)
            else:
                m_ahead = scores(nslot, 0, nh, (j + 1) % 2)
            m_new = jnp.maximum(m_run, jnp.max(m_blk, axis=0, keepdims=True))
            alpha = jnp.exp2((m_run - m_new) * cexp)
            p = jnp.exp2((sbuf[j % 2] - m_new) * cexp)
            l_run = l_run * alpha + jnp.sum(p.reshape(kblk // 8, 8, tok), axis=0)
            o_run = o_run * alpha + jnp.dot(vb[slot, :, pl.ds(j * kblk, kblk)], p.astype(jnp.bfloat16),
                                            preferred_element_type=jnp.float32)
            m_run = m_new
        mst[h] = jnp.broadcast_to(m_run, (8, tok))
        lst[h] = l_run
        acc[h] = o_run

        @pl.when(slot == 7)
        def _():
            o = acc[h] / jnp.sum(lst[h], axis=0, keepdims=True)
            ost[:, pl.ds(pl.multiple_of(h * HD, HD), HD)] = o.T.astype(jnp.bfloat16)

        return m_ahead

    lax.fori_loop(0, 8 * group, step, m_first)
    for p in range(1, 8):
        ck, cv = remote(p)
        ck.wait_send()
        cv.wait_send()
    send_out(group - 1)

    def cols_of(p):
        return og_ref.at[:, pl.ds(pl.multiple_of(head_of(p) * width, width), width)]

    def forward(n, p):
        return pltpu.make_async_remote_copy(cols_of(p), cols_of(p), fsend.at[n], frecv.at[n],
                                            device_id=dev(1), device_id_type=pl.DeviceIdType.MESH)

    for n, p in enumerate((3, 2, 6)):
        pltpu.make_async_copy(cols_of(p), cols_of(p), orecv.at[p]).wait()
        forward(n, p).start()
    pltpu.make_async_copy(cols_of(1), cols_of(1), orecv.at[1]).wait()
    for p in (0, 1, 2, 3, 6):
        pltpu.make_async_copy(ost.at[pl.ds(0, half), :], ost.at[pl.ds(0, half), :], osend.at[p]).wait()
    for n, p in enumerate((3, 2, 6)):
        forward(n, p).wait()


def attention(kh, vh, qt, kn, vnt, kblk=2048):
    n_kv, cache, _ = kh.shape
    group, tok = qt.shape[0] // HD, qt.shape[1]
    return pl.pallas_call(
        functools.partial(attn_kernel, tok=tok, group=group, kblk=kblk, scale=HD ** -0.5),
        in_specs=[pl.BlockSpec(memory_space=pl.ANY), pl.BlockSpec(memory_space=pl.ANY)] + [pl.BlockSpec(memory_space=pltpu.VMEM)] * 3,
        out_specs=pl.BlockSpec(memory_space=pl.ANY),
        out_shape=jax.ShapeDtypeStruct((tok // 2, n_kv * group * HD), jnp.bfloat16),
        scratch_shapes=[
            pltpu.VMEM((8, cache, HD), jnp.bfloat16),
            pltpu.VMEM((8, HD, cache), jnp.bfloat16),
            pltpu.VMEM((2, kblk, tok), jnp.float32),
            pltpu.VMEM((group, HD, tok), jnp.float32),
            pltpu.VMEM((group, 8, tok), jnp.float32),
            pltpu.VMEM((group, 8, tok), jnp.float32),
            pltpu.VMEM((tok, group * HD), jnp.bfloat16),
        ] + [pltpu.SemaphoreType.DMA((8,))] * 6 + [pltpu.SemaphoreType.DMA((3,))] * 2,
        compiler_params=pltpu.CompilerParams(collective_id=0, has_side_effects=True, vmem_limit_bytes=62 << 20),
    )(kh, vh, qt, kn, vnt)


def oproj_kernel(x_hbm, w_hbm, y_hbm, x_ref, wbuf, yst, xsem, wsem, ysend, yrecv, *, bn, rows):
    sp, cp = lax.axis_index('sp'), lax.axis_index('cp')
    chip, core = cp // 2, cp % 2
    steps, n_buf = yst.shape[0], wbuf.shape[0]
    base = cp * (steps * bn)

    def dev(f):
        c = (1 - chip if f // 2 else chip) * 2 + (1 - core if f % 2 else core)
        return c, {'sp': sp, 'cp': c}

    barrier = pltpu.get_barrier_semaphore()
    for f in range(1, 4):
        pl.semaphore_signal(barrier, inc=1, device_id=dev(f)[1], device_id_type=pl.DeviceIdType.MESH)

    def wcopy(n, slot):
        cols = pl.ds(pl.multiple_of(base + n * bn, bn), bn)
        return pltpu.make_async_copy(w_hbm.at[:, cols], wbuf.at[slot], wsem.at[slot])

    xc = pltpu.make_async_copy(x_hbm, x_ref, xsem)
    xc.start()
    for n in range(n_buf):
        wcopy(n, n).start()
    pl.semaphore_wait(barrier, 3)
    xc.wait()

    def y_copies(n):
        cols = pl.ds(pl.multiple_of(base + n * bn, bn), bn)
        res = [pltpu.make_async_copy(yst.at[n, pl.ds(cp * rows, rows), :], y_hbm.at[:, cols], ysend.at[0])]
        for f in range(1, 4):
            c, d = dev(f)
            res.append(pltpu.make_async_remote_copy(yst.at[n, pl.ds(c * rows, rows), :], y_hbm.at[:, cols], ysend.at[f], yrecv.at[f],
                                                    device_id=d, device_id_type=pl.DeviceIdType.MESH))
        return res

    def send(n):
        for c in y_copies(n):
            c.start()

    def step(n, carry):
        slot = n % n_buf
        wcopy(n, slot).wait()
        yst[n] = jnp.dot(x_ref[...], wbuf[slot], preferred_element_type=jnp.float32).astype(jnp.bfloat16)

        @pl.when(n + n_buf < steps)
        def _():
            wcopy(n + n_buf, slot).start()

        @pl.when(n > 0)
        def _():
            send(n - 1)

        return carry

    lax.fori_loop(0, steps, step, 0)
    send(steps - 1)
    width = steps * bn
    for f in range(4):
        c, _ = dev(f)
        mine = y_hbm.at[:, pl.ds(pl.multiple_of(c * width, width), width)]
        pltpu.make_async_copy(mine, mine, ysend.at[f]).wait()
        if f:
            pltpu.make_async_copy(mine, mine, yrecv.at[f]).wait()


def out_project(o_g, w_o, cp_size, bn=256):
    rows, depth = o_g.shape
    n_cols = w_o.shape[1]
    steps = n_cols // cp_size // bn
    return pl.pallas_call(
        functools.partial(oproj_kernel, bn=bn, rows=rows // cp_size),
        in_specs=[pl.BlockSpec(memory_space=pl.ANY)] * 2,
        out_specs=pl.BlockSpec(memory_space=pl.ANY),
        out_shape=jax.ShapeDtypeStruct((rows // cp_size, n_cols), jnp.bfloat16),
        scratch_shapes=[
            pltpu.VMEM((rows, depth), jnp.bfloat16),
            pltpu.VMEM((4, depth, bn), jnp.bfloat16),
            pltpu.VMEM((steps, rows, bn), jnp.bfloat16),
            pltpu.SemaphoreType.DMA,
            pltpu.SemaphoreType.DMA((4,)),
            pltpu.SemaphoreType.DMA((4,)),
            pltpu.SemaphoreType.DMA((4,)),
        ],
        compiler_params=pltpu.CompilerParams(collective_id=1, has_side_effects=True, vmem_limit_bytes=60 << 20),
    )(o_g, w_o)


def solution(mesh):
    cp_size = mesh.shape['cp']
    row_spec = P(('dp', 'sp', 'cp'))

    def local_fn(x_loc, kc_loc, vc_loc, w_q, w_k, w_v, w_o):
        cache_loc, n_kv, _ = kc_loc.shape
        seq_size = mesh.shape['sp'] * cp_size
        sp = lax.axis_index('sp')
        rows = x_loc.shape[0] * cp_size
        cos_t, sin_t = rope_tables(cache_loc * seq_size + sp * rows + jnp.arange(rows))
        qt, kv_rows, kv_head = front(x_loc, w_q, w_k, w_v, cos_t, sin_t, cp_size)
        k_new = kv_rows[0].reshape(x_loc.shape[0], n_kv, HD)
        v_new = kv_rows[1].reshape(x_loc.shape[0], n_kv, HD)
        qt, kc_loc, vc_loc = lax.optimization_barrier((qt, kc_loc, vc_loc))
        qt = lax.all_to_all(qt, 'sp', split_axis=0, concat_axis=1, tiled=True)
        kh = jnp.transpose(kc_loc, (1, 0, 2))
        vh = jnp.transpose(vc_loc, (1, 2, 0))
        o_g = attention(kh, vh, qt, kv_head[0], kv_head[1].T)
        y_loc = out_project(o_g, w_o, cp_size, BN_O)
        return y_loc, k_new, v_new

    return jax.shard_map(local_fn, mesh=mesh, in_specs=(row_spec, row_spec, row_spec, P(), P(), P(), P()), out_specs=(row_spec, row_spec, row_spec), check_vma=False)
```
